32 devices in a mesh: groups: 2 (over y), ep: 4 (over x, core), tp: 4 (over z).
Axes of the slice: x: 2, y: 2, z: 4, core: 2. Of those that a mesh axis runs over, the one named last changes fastest.
Arguments:
- tokens: bfloat16 [256, 7168], P(('groups', 'ep')), parts along dimension 0, may hold values from -6 to 6
- w_gate: bfloat16 [16, 7168, 2048], P('ep', None, 'tp'), may hold values from -0.0625 to 0.0625
- w_up: bfloat16 [16, 7168, 2048], P('ep', None, 'tp'), may hold values from -0.0625 to 0.0625
- w_down: bfloat16 [16, 2048, 7168], P('ep', 'tp'), may hold values from -0.1875 to 0.1875
- router_logits: float32 [256, 8], P(('groups', 'ep')), parts along dimension 0, may hold values from -6 to 6
- expert_ids: int32 [256, 8], P(('groups', 'ep')), parts along dimension 0, may hold values from 0 to 15, all different within a row; in each aligned block of 32 rows (0 to 31, 32 to 63, ...) at most 24 rows name the same one
- draft_lengths: int32 [32], P(('groups', 'ep')), parts along dimension 0, may hold values from 7 to 8
- accept_mask: int32 [32, 8], P(('groups', 'ep')), parts along dimension 0, may hold values 0 or 1
Outputs:
- mixed: bfloat16 [256, 7168], P(('groups', 'ep'), 'tp'), parts along dimension 0
- accepted: int32 [2], P('groups'), parts along dimension 0
The draws below stay inside these ranges and needn't reach their ends.
There are 2 independent parts, one for each index of `groups`. The reference program is written for one: setup_inputs(seed, part) draws one part's arguments, and reference() takes and returns one part's arrays. A program takes and returns all parts, laid end to end along the dimension named above; an argument that names none is the same for every part. Nothing has to cross between parts.
Inputs may be any that keep to these rules, and one draw needn't show every extreme that they name: `expert_ids`: each row names 8 different experts. Among the rows of one ep index (aligned blocks of 32 rows) no expert is named by more than 24 rows, and in every draw some expert is named by exactly 24 rows of some block.
All inputs are finite; a program needn't handle non-finite values. No bound on the sum of `accept_mask` on one device may be relied on, other than what follows from the above.
Results may differ from the reference program's by a relative error of at most 0.017.
Values may be sent and summed in bfloat16 or wider, within the bound.
A program may use at most 192 MiB of HBM per device.

```python
import math
import jax
import jax.numpy as jnp
import numpy as np
from jax import lax

D = 7168
FF = 2048
TOP = 8
DRAFT = 8
EXPERTS = 16
TOK_DEV = 32
REQUESTS = 16
TOKENS = 128
CAP = 24
N_EP = 4
N_TP = 4


def set_ends(result, own_key, smallest, high):
    shape = result.shape
    spot = [jax.random.randint(jax.random.fold_in(own_key, axis), (), 0, shape[axis]) for axis in range(len(shape))]
    result = result.at[tuple(spot)].set(smallest)
    longest = shape.index(max(shape))
    spot[longest] = (spot[longest] + 1) % shape[longest]
    return result.at[tuple(spot)].set(high)


def raised(entries, rng, source, target, blocks, factor):
    owner, partner = [(jnp.arange(entries.shape[position]) // (entries.shape[position] // blocks)).reshape([-1 if axis == position else 1 for axis in range(entries.ndim)]) for position in (source, target)]
    chosen = jax.random.permutation(rng, blocks)[partner]
    strong = (owner == chosen) | (owner == (partner + blocks // 2) % blocks)
    return jnp.where(strong, factor * entries, entries)


def block_levels(own_key, extent, shards, low, high):
    gain, own = 1.0, jax.random.fold_in(own_key, 6)
    for axis_at, blocks in shards:
        draws = jnp.exp(jax.random.uniform(jax.random.fold_in(own, axis_at), (blocks,), jnp.float32, low / len(shards), high / len(shards)))
        gain = gain * jnp.repeat(draws, extent[axis_at] // blocks).reshape([-1 if axis == axis_at else 1 for axis in range(len(extent))])
    return gain


def shared_out(own_key, own, number, rows, count, top, reach, lean):
    order = jax.random.permutation(own_key, count)
    heavy_load, common = shares(count, rows * top, reach, lean, True), shares(count, rows * top, reach, lean, False)
    places = jnp.arange(count)

    def named(tallies, rotation):
        used = int((tallies > 0).sum())
        fixed = max(1, used // 4)
        shifted = fixed + (places - fixed + rotation * (used - fixed)) % max(1, count - fixed)
        return jnp.zeros((count,), jnp.int32).at[order[jnp.where(places < fixed, places, shifted)]].set(jnp.asarray(tallies, jnp.int32))

    tallies = jnp.where(number % 4 == 0, named(heavy_load, number // 4), named(common, number - number // 4 - 1))
    mixed = jax.random.permutation(jax.random.fold_in(own, 3), count)
    giver, taker = mixed[0:count // 2 * 2:2], mixed[1:count // 2 * 2:2]
    slack = jnp.minimum(tallies[giver] - 1, reach - tallies[taker]) // 2
    slack = jnp.where((giver == order[0]) | (taker == order[0]) | (tallies[taker] == 0), 0, jnp.maximum(slack, 0))
    shifted = jax.random.randint(jax.random.fold_in(own, 4), (count // 2,), 0, 1 << 20) % (slack + 1)
    tallies = tallies.at[giver].add(-shifted).at[taker].add(shifted)
    labels = jnp.searchsorted(jnp.cumsum(tallies), jnp.arange(rows * top), side="right").astype(jnp.int32)
    listing = labels.reshape(top, rows).T
    listing = listing[jax.random.permutation(jax.random.fold_in(own, 1), rows)]
    rotation = jax.random.randint(jax.random.fold_in(own, 2), (rows, 1), 0, top)
    return jnp.take_along_axis(listing, (jnp.arange(top)[None, :] + rotation) % top, axis=1)


def shares(amount, total, limit, skew, full):
    loads = [(1 << 20) // math.isqrt(rank ** skew) + 1 for rank in range(1, amount + 1)]
    largest = limit if full else min(limit, max(-(-total // amount), total * loads[0] // sum(loads)))
    least = 1 if total - largest >= amount - 1 else 0
    given, surplus = [largest] + [least] * (amount - 1), total - largest - least * (amount - 1)
    while surplus > 0:
        movable = [i for i in range(1, amount) if given[i] < largest] or [i for i in range(1, amount) if given[i] < limit]
        whole, remaining = sum([loads[i] for i in movable]), surplus
        for i in movable:
            extra = min(limit - given[i], max(1, remaining * loads[i] // whole), surplus)
            given[i] = given[i] + extra
            surplus = surplus - extra
    return np.array(given)


def bell_draw(stream_key, shape, scale, bound, shards=(), held_as=jnp.bfloat16):
    values = jax.random.normal(stream_key, shape, jnp.float32) * scale
    if len(shards) > 0:
        values = block_levels(stream_key, shape, shards, -0.22, 0.18) * values
    return jnp.clip(values, min=-bound, max=bound).astype(held_as)


def gaussian_with(rng, shape, deviation, bound, shards, heavy, kind=jnp.bfloat16):
    drawn = deviation * jax.random.normal(rng, shape, jnp.float32)
    if shards:
        drawn = drawn * block_levels(rng, shape, shards, -0.22, 0.18)
    return jnp.clip(raised(drawn, jax.random.fold_in(rng, 3), *heavy), -bound, bound).astype(kind)


def setup_inputs(seed: int = 0, part: int = 0) -> dict:
    arg_keys = jax.random.split(jax.random.key(seed), 9)
    own_keys = jax.random.split(jax.random.fold_in(arg_keys[8], part), 9)
    tokens = bell_draw(own_keys[0], (TOKENS, D), 1.0, 6.0, ((0, 4),))
    w_gate = bell_draw(arg_keys[1], (EXPERTS, D, FF), D ** -0.5, 0.0625, ((0, 4), (2, 4)))
    w_up = bell_draw(arg_keys[2], (EXPERTS, D, FF), D ** -0.5, 0.0625, ((0, 4), (2, 4)))
    w_down = gaussian_with(arg_keys[3], (EXPERTS, FF, D), FF ** -0.5, 0.1875, ((0, 4), (1, 4)), (1, 2, 4, 2.0))
    router_logits = bell_draw(own_keys[4], (TOKENS, TOP), 1.5, 6.0, ((0, 4),), jnp.float32)
    expert_ids_keys = jax.random.split(jax.random.fold_in(own_keys[5], 1), TOKENS // TOK_DEV)
    expert_ids_turns = jax.random.permutation(jax.random.fold_in(own_keys[5], 3), TOKENS // TOK_DEV)
    expert_ids = jax.vmap(lambda own, number: shared_out(jax.random.fold_in(own_keys[5], 2), own, number, TOK_DEV, EXPERTS, TOP, CAP, 2))(expert_ids_keys, expert_ids_turns).reshape((TOKENS, TOP))
    draft_lengths = set_ends(jax.random.randint(own_keys[6], (REQUESTS,), DRAFT - 1, DRAFT + 1), jax.random.fold_in(own_keys[6], 1), DRAFT - 1, DRAFT).astype(jnp.int32)
    accept_mask = set_ends((jax.random.randint(own_keys[7], (REQUESTS, DRAFT), 0, 4) < 3).astype(jnp.int32), jax.random.fold_in(own_keys[7], 1), 0, 1)
    return dict(tokens=tokens, w_gate=w_gate, w_up=w_up, w_down=w_down, router_logits=router_logits, expert_ids=expert_ids, draft_lengths=draft_lengths, accept_mask=accept_mask)


def reference(tokens, w_gate, w_up, w_down, router_logits, expert_ids, draft_lengths, accept_mask):
    live = jnp.arange(DRAFT, dtype=jnp.int32)[None, :] < draft_lengths[:, None]
    live_rows = live.reshape(TOKENS)
    live_tokens = jnp.where(live_rows[:, None], tokens, jnp.zeros((), tokens.dtype))
    sig = jax.nn.sigmoid(router_logits.astype(jnp.float32))
    gates = 2.827 * sig / jnp.sum(sig, axis=1, keepdims=True)
    load = N_EP * CAP
    flat_ids = expert_ids.reshape(-1).astype(jnp.int32)
    onehot = (flat_ids[:, None] == jnp.arange(EXPERTS, dtype=jnp.int32)[None, :]).astype(jnp.int32)
    rank = jnp.cumsum(onehot, axis=0) - 1
    slot = jnp.sum(rank * onehot, axis=1).astype(jnp.int32)
    source = (jnp.arange(TOKENS * TOP, dtype=jnp.int32) // TOP).astype(jnp.int32)
    table = jnp.zeros((EXPERTS, load), jnp.int32).at[flat_ids, slot].set(source)
    filled = jnp.zeros((EXPERTS, load), jnp.int32).at[flat_ids, slot].set(1)

    def one_expert(items):
        weight_g, weight_u, weight_d, rows_of, used = items
        rows = jnp.where(used[:, None] > 0, live_tokens[rows_of], jnp.zeros((), tokens.dtype))
        gate = jnp.dot(rows, weight_g, preferred_element_type=jnp.float32)
        up = jnp.dot(rows, weight_u, preferred_element_type=jnp.float32)
        hidden = (jax.nn.silu(gate) * up).astype(jnp.bfloat16)
        blocks = hidden.reshape(load, N_TP, FF // N_TP).astype(jnp.float32)
        down = weight_d.reshape(N_TP, FF // N_TP, D).astype(jnp.float32)
        parts = jnp.einsum('mtf,tfd->tmd', blocks, down)
        summed = jnp.sum(parts.astype(jnp.bfloat16).astype(jnp.float32), axis=0)
        return summed.astype(jnp.bfloat16)

    outs = lax.map(one_expert, (w_gate, w_up, w_down, table, filled))
    picked = outs[flat_ids, slot].reshape(TOKENS, TOP, D).astype(jnp.float32)
    mixed = jnp.sum(gates[:, :, None] * picked, axis=1).astype(jnp.bfloat16)
    passed = accept_mask.astype(jnp.int32) * live.astype(jnp.int32)
    prefix = jnp.cumprod(passed, axis=1)
    accepted = jnp.sum(prefix).astype(jnp.int32).reshape(1)
    return mixed, accepted
```

```python
import jax
import jax.numpy as jnp
from jax import lax
from jax.sharding import PartitionSpec as P

DRAFT = 8
EXPERTS = 16


def per_device(tokens, w_gate, w_up, w_down, router_logits, expert_ids, draft_lengths, accept_mask):
    tok_rows = tokens.shape[0]
    local = w_gate.shape[0]
    me = lax.axis_index("ep")
    live = jnp.arange(DRAFT, dtype=jnp.int32)[None, :] < draft_lengths[:, None]
    sig = jax.nn.sigmoid(router_logits)
    gates = 2.827 * sig / jnp.sum(sig, axis=1, keepdims=True)
    named = expert_ids[:, :, None] == jnp.arange(EXPERTS, dtype=jnp.int32)[None, None, :]
    dense = jnp.sum(jnp.where(named, gates[:, :, None], 0.0), axis=1)
    dense = jnp.where(live.reshape(tok_rows)[:, None], dense, 0.0)
    rows = lax.all_gather(tokens, "ep", axis=0, tiled=True)
    dense = lax.all_gather(dense, "ep", axis=0, tiled=True)
    mine = lax.dynamic_slice_in_dim(dense, me * local, local, axis=1)
    gate = jnp.einsum("md,edf->emf", rows, w_gate, preferred_element_type=jnp.float32)
    up = jnp.einsum("md,edf->emf", rows, w_up, preferred_element_type=jnp.float32)
    hidden = (jax.nn.silu(gate) * up * mine.T[:, :, None]).astype(jnp.bfloat16)
    partial = jnp.einsum("emf,efd->md", hidden, w_down, preferred_element_type=jnp.float32)
    partial = partial.astype(jnp.bfloat16)
    partial = lax.psum_scatter(partial, "ep", scatter_dimension=0, tiled=True)
    mixed = lax.psum_scatter(partial, "tp", scatter_dimension=1, tiled=True)
    passed = accept_mask * live.astype(jnp.int32)
    accepted = lax.psum(jnp.sum(jnp.cumprod(passed, axis=1)), "ep").reshape(1)
    return (mixed, accepted)


def solution(mesh):
    placed = (
        P(("groups", "ep"), None),
        P("ep", None, "tp"),
        P("ep", None, "tp"),
        P("ep", "tp", None),
        P(("groups", "ep"), None),
        P(("groups", "ep"), None),
        P(("groups", "ep")),
        P(("groups", "ep"), None),
    )
    return jax.shard_map(
        per_device,
        mesh=mesh,
        in_specs=placed,
        out_specs=(P(("groups", "ep"), "tp"), P("groups")),
        check_vma=False,
    )
```

```python
import functools

import jax
import jax.numpy as jnp
from jax import lax
from jax.experimental import pallas as pl
from jax.experimental.pallas import tpu as pltpu
from jax.sharding import PartitionSpec as P

DRAFT = 8
EXPERTS = 16
LANES = 128
MESH = pl.DeviceIdType.MESH


def kernel(n_ep, n_tp, pieces, slots, lens, tokens, logits, ids, mask, wg, wu, wd,
           out, count, xbuf, gbuf, wgb, wub, wdb, accg, accu, hid, pbuf, r1, s1, r2, s2, r3, own,
           gsem, usem, dsem, xr, xs, ps, fs, s1s, s1r, s2s, s2r, s3s, s3r):
    me, tp = lax.axis_index("ep"), lax.axis_index("tp")
    chip, core = me // 2, me % 2
    n_chip = n_ep // 2
    partner = me + 1 - 2 * core
    rows, width = tokens.shape
    local, _, ff = wg.shape
    kc = width // pieces
    cols = width // n_tp
    total_rows = n_ep * rows
    steps = pieces * local

    def gu(s, slot):
        e, at = s % local, pl.multiple_of((s // local) * kc, kc)
        return (pltpu.make_async_copy(wg.at[e, pl.ds(at, kc), :], wgb.at[slot], gsem.at[slot]),
                pltpu.make_async_copy(wu.at[e, pl.ds(at, kc), :], wub.at[slot], usem.at[slot]))

    def down(j):
        z = lax.rem(tp + 1 + j, n_tp)
        return pltpu.make_async_copy(wd.at[:, :, pl.ds(pl.multiple_of(z * cols, cols), cols)], wdb.at[j], dsem.at[j])

    for s in range(slots):
        for c in gu(s, s):
            c.start()

    sig = 1.0 / (1.0 + jnp.exp(-logits[...]))
    gates = 2.827 * sig / jnp.sum(sig, axis=1, keepdims=True)
    lane = lax.broadcasted_iota(jnp.int32, (rows, LANES), 1)
    row = lax.broadcasted_iota(jnp.int32, (rows, LANES), 0)
    dense = jnp.zeros((rows, LANES), jnp.float32)
    named = ids[...]
    for k in range(logits.shape[1]):
        dense = dense + jnp.where(named[:, k:k + 1] == lane, gates[:, k:k + 1], 0.0)
    requests = mask.shape[0]
    end = jnp.zeros((rows, LANES), jnp.int32)
    short = jnp.zeros((requests, DRAFT), jnp.int32)
    request = lax.broadcasted_iota(jnp.int32, (requests, DRAFT), 0)
    draft = lax.broadcasted_iota(jnp.int32, (requests, DRAFT), 1)
    for r in range(requests):
        end = jnp.where(row >= r * DRAFT, r * DRAFT + lens[r], end)
        short = jnp.where(request == r, lens[r], short)
    dense = jnp.where(row < end, dense, 0.0)
    passed = jnp.where(draft < short, mask[...], 0).astype(jnp.float32)
    run = passed[:, 0:1]
    kept = run
    for j in range(1, DRAFT):
        run = run * passed[:, j:j + 1]
        kept = kept + run
    gbuf[me] = jnp.where(lane == EXPERTS, jnp.sum(kept), dense)
    xbuf[me] = tokens[...]

    peers = [lax.rem(chip + d, n_chip) * 2 + core for d in range(1, n_chip)]
    sources = [lax.rem(chip + n_chip - d, n_chip) * 2 + core for d in range(1, n_chip)]
    barrier = pltpu.get_barrier_semaphore()
    for peer in peers + [partner]:
        pl.semaphore_signal(barrier, inc=1, device_id={"ep": peer}, device_id_type=MESH)
    for d in range(1, n_tp):
        pl.semaphore_signal(barrier, inc=1, device_id={"tp": lax.rem(tp + d, n_tp)}, device_id_type=MESH)
    pl.semaphore_wait(barrier, n_chip + n_tp - 1)

    def view(source, p):
        if p == pieces:
            return gbuf.at[source]
        return xbuf.at[source, :, pl.ds(p * kc, kc)]

    def move(source, p, send, target):
        src = view(source, p)
        if p < pieces and source is me:
            src = tokens.at[:, pl.ds(p * kc, kc)]
        return pltpu.make_async_remote_copy(src_ref=src, dst_ref=view(source, p), send_sem=send,
                                            recv_sem=xr.at[source, p], device_id={"ep": target}, device_id_type=MESH)

    sends = []
    order = [0, pieces] + list(range(1, pieces))
    for p in order:
        for d, peer in enumerate(peers):
            sends.append(move(me, p, xs.at[d, p], peer))
            sends[-1].start()
        sends.append(move(me, p, ps.at[p], partner))
        sends[-1].start()

    def forward(p):
        for d, source in enumerate(sources):
            move(source, p, xs.at[d, p], partner).wait_recv()
            sends.append(move(source, p, fs.at[d, p], partner))
            sends[-1].start()

    def landed(p):
        move(partner, p, ps.at[p], partner).wait_recv()
        for source in sources:
            move(source + 1 - 2 * core, p, ps.at[p], partner).wait_recv()

    forward(0)
    forward(pieces)
    for p in range(pieces):
        if p + 1 < pieces:
            forward(p + 1)
        for j in range(n_tp):
            if max(0, pieces - n_tp + j) == p:
                down(j).start()
        landed(p)

        @pl.loop(0, local)
        def _(e):
            s = p * local + e
            slot = lax.rem(s, slots)
            for c in gu(s, slot):
                c.wait()
            x = xbuf[:, :, p * kc:(p + 1) * kc].reshape(total_rows, kc)
            g = jnp.dot(x, wgb[slot], preferred_element_type=jnp.float32)
            u = jnp.dot(x, wub[slot], preferred_element_type=jnp.float32)
            if p == 0:
                accg[e] = g
                accu[e] = u
            else:
                accg[e] += g
                accu[e] += u
            if (p + 1) * local - 1 + slots < steps or p * local + slots < steps:
                @pl.when(s + slots < steps)
                def _():
                    for c in gu(s + slots, slot):
                        c.start()
    landed(pieces)

    dense = gbuf[...].reshape(total_rows, LANES)
    lane = lax.broadcasted_iota(jnp.int32, (total_rows, LANES), 1)
    for e in range(local):
        gate = jnp.sum(jnp.where(lane == me * local + e, dense, 0.0), axis=1, keepdims=True)
        v = accg[e]
        hid[:, e * ff:(e + 1) * ff] = (v / (1.0 + jnp.exp(-v)) * accu[e] * gate).astype(jnp.bfloat16)

    def first(j):
        return pltpu.make_async_remote_copy(
            src_ref=pbuf.at[j, :, 1 - core], dst_ref=r1.at[j], send_sem=s1s.at[j], recv_sem=s1r.at[j],
            device_id={"ep": partner}, device_id_type=MESH)

    def second(j, d):
        to = lax.rem(chip + d, n_chip)
        return pltpu.make_async_remote_copy(
            src_ref=s1.at[j, to], dst_ref=r2.at[j, d - 1], send_sem=s2s.at[j, d - 1], recv_sem=s2r.at[j, d - 1],
            device_id={"ep": to * 2 + core}, device_id_type=MESH)

    def third(j):
        return pltpu.make_async_remote_copy(
            src_ref=s2.at[j], dst_ref=r3.at[j], send_sem=s3s.at[j], recv_sem=s3r.at[j],
            device_id={"tp": lax.rem(tp + 1 + j, n_tp)}, device_id_type=MESH)

    def stage2(j):
        first(j).wait_recv()
        s1[j] = (pbuf[j, :, core].astype(jnp.float32) + r1[j].astype(jnp.float32)).astype(jnp.bfloat16)
        for d in range(1, n_chip):
            second(j, d).start()

    def stage3(j):
        value = s1[j, chip].astype(jnp.float32)
        for d in range(1, n_chip):
            second(j, d).wait_recv()
            value = value + r2[j, d - 1].astype(jnp.float32)
        if j < n_tp - 1:
            s2[j] = value.astype(jnp.bfloat16)
            third(j).start()
        else:
            own[...] = value

    for j in range(n_tp):
        down(j).wait()
        y = jnp.dot(hid[...], wdb[j].reshape(local * ff, cols), preferred_element_type=jnp.float32)
        pbuf[j] = y.astype(jnp.bfloat16).reshape(n_chip, 2, rows, cols)
        first(j).start()
        if j >= 2:
            stage3(j - 2)
        if j >= 1:
            stage2(j - 1)
    if n_tp >= 2:
        stage3(n_tp - 2)
    stage2(n_tp - 1)
    stage3(n_tp - 1)

    rowid = lax.broadcasted_iota(jnp.int32, (rows, LANES), 0)
    lane = lax.broadcasted_iota(jnp.int32, (rows, LANES), 1)
    tally = jnp.zeros((rows, LANES), jnp.float32)
    for i in range(n_ep):
        tally = tally + gbuf[i]
    count[0] = jnp.sum(jnp.where((rowid == 0) & (lane == EXPERTS), tally, 0.0)).astype(jnp.int32)

    value = own[...]
    for j in range(n_tp - 1):
        third(j).wait_recv()
        value = value + r3[j].astype(jnp.float32)
    out[...] = value.astype(jnp.bfloat16)

    for c in sends:
        c.wait_send()
    for j in range(n_tp):
        first(j).wait_send()
        for d in range(1, n_chip):
            second(j, d).wait_send()
        if j < n_tp - 1:
            third(j).wait_send()


def per_device(n_ep, n_tp, tokens, w_gate, w_up, w_down, router_logits, expert_ids, draft_lengths, accept_mask):
    rows, width = tokens.shape
    local, _, ff = w_gate.shape
    n_chip = n_ep // 2
    pieces = 7 if width % (7 * LANES) == 0 else 1
    kc, cols = width // pieces, width // n_tp
    slots = min(8, pieces * local)
    vmem, hbm, smem = [pl.BlockSpec(memory_space=m) for m in (pltpu.VMEM, pl.ANY, pltpu.SMEM)]
    bf, f32, dma = jnp.bfloat16, jnp.float32, pltpu.SemaphoreType.DMA
    back = max(1, n_chip - 1)
    return pl.pallas_call(
        functools.partial(kernel, n_ep, n_tp, pieces, slots),
        out_shape=(jax.ShapeDtypeStruct((rows, cols), bf), jax.ShapeDtypeStruct((1,), jnp.int32)),
        in_specs=[smem, vmem, vmem, vmem, vmem, hbm, hbm, hbm],
        out_specs=(vmem, smem),
        scratch_shapes=[
            pltpu.VMEM((n_ep, rows, width), bf),
            pltpu.VMEM((n_ep, rows, LANES), f32),
            pltpu.VMEM((slots, kc, ff), bf),
            pltpu.VMEM((slots, kc, ff), bf),
            pltpu.VMEM((n_tp, local, ff, cols), bf),
            pltpu.VMEM((local, n_ep * rows, ff), f32),
            pltpu.VMEM((local, n_ep * rows, ff), f32),
            pltpu.VMEM((n_ep * rows, local * ff), bf),
            pltpu.VMEM((n_tp, n_chip, 2, rows, cols), bf),
            pltpu.VMEM((n_tp, n_chip, rows, cols), bf),
            pltpu.VMEM((n_tp, n_chip, rows, cols), bf),
            pltpu.VMEM((n_tp, back, rows, cols), bf),
            pltpu.VMEM((n_tp, rows, cols), bf),
            pltpu.VMEM((n_tp, rows, cols), bf),
            pltpu.VMEM((rows, cols), f32),
            dma((slots,)), dma((slots,)), dma((n_tp,)),
            dma((n_ep, pieces + 1)), dma((back, pieces + 1)), dma((pieces + 1,)), dma((back, pieces + 1)),
            dma((n_tp,)), dma((n_tp,)), dma((n_tp, back)), dma((n_tp, back)), dma((n_tp,)), dma((n_tp,)),
        ],
        compiler_params=pltpu.CompilerParams(
            collective_id=0, has_side_effects=True, vmem_limit_bytes=66_000_000),
    )(draft_lengths, tokens, router_logits, expert_ids, accept_mask, w_gate, w_up, w_down)


def solution(mesh):
    placed = (
        P(("groups", "ep"), None),
        P("ep", None, "tp"),
        P("ep", None, "tp"),
        P("ep", "tp", None),
        P(("groups", "ep"), None),
        P(("groups", "ep"), None),
        P(("groups", "ep")),
        P(("groups", "ep"), None),
    )
    return jax.shard_map(
        functools.partial(per_device, mesh.shape["ep"], mesh.shape["tp"]),
        mesh=mesh,
        in_specs=placed,
        out_specs=(P(("groups", "ep"), "tp"), P("groups")),
        check_vma=False,
    )
```
